32 devices in a mesh: groups: 2 (over y), seq: 4 (over z), batch: 2 (over x), head: 2 (over core).
Axes of the slice: x: 2, y: 2, z: 4, core: 2. Of those that a mesh axis runs over, the one named last changes fastest.
Arguments:
- hidden_in: bfloat16 [64, 4096], P(('groups', 'batch'), 'seq'), parts along dimension 0, may hold values from -400 to 400
- norm_gain_vector: bfloat16 [4096], P('seq'), may hold values from 0.099609375 to 1.8984375
- w_query: bfloat16 [4096, 4096], P('seq', 'head'), may hold values from -0.09375 to 0.09375
- key_cache_rows: bfloat16 [64, 4096, 128], P(('groups', 'batch'), 'seq'), parts along dimension 0, may hold values from -360 to 360
- value_cache_rows: bfloat16 [64, 4096, 128], P(('groups', 'batch'), 'seq'), parts along dimension 0, may hold values from -6 to 6
- k_new: bfloat16 [64, 128], P(('groups', 'batch')), parts along dimension 0, may hold values from -360 to 360
- v_new: bfloat16 [64, 128], P(('groups', 'batch')), parts along dimension 0, may hold values from -6 to 6
- lengths: int32 [64], P(('groups', 'batch')), parts along dimension 0, may hold values from 1 to 4096, as said below
- w_out: bfloat16 [4096, 4096], P('head', 'seq'), may hold values from -0.09375 to 0.09375
Outputs:
- layer_out: float32 [64, 4096], P(('groups', 'batch'), ('seq', 'head')), parts along dimension 0
The draws below stay inside these ranges and needn't reach their ends.
There are 2 independent parts, one for each index of `groups`. The reference program is written for one: setup_inputs(seed, part) draws one part's arguments, and reference() takes and returns one part's arrays. A program takes and returns all parts, laid end to end along the dimension named above; an argument that names none is the same for every part. Nothing has to cross between parts.
Inputs may be any that keep to these rules, and one draw needn't show every extreme that they name: `lengths`: every sequence has at least one cached position; some sequence of each draw uses all 4096.
All inputs are finite; a program needn't handle non-finite values.
Results may differ from the reference program's by a relative error of at most 0.008.
Values sent between devices are 32-bit elements; how exact they have to be, the bound alone decides.
A program may use at most 64 MiB of HBM per device.

```python
import jax
import jax.numpy as jnp
from jax import lax

D = 4096
HQ = 32
HD = 128
B = 32
CTX = 4096
QW = 4096


def drawn_keys(key, shape):
    values = jnp.clip(jax.random.normal(key, shape, jnp.float32), -6.0, 6.0) * 2.5
    return values


def draw_key_cache_rows(key, part):
    values = drawn_keys(jax.random.fold_in(key, 1), (B, CTX, HD))
    return values.astype(jnp.bfloat16)


def draw_k_new(key, part):
    values = drawn_keys(jax.random.fold_in(key, 2), (B, HD))
    return values.astype(jnp.bfloat16)


def draw_hidden_in(key, part):
    first, second, third = jax.random.split(jax.random.fold_in(key, 3), 3)
    base = jnp.clip(jax.random.normal(first, (B, D), jnp.float32), -4.0, 4.0)
    row_scale = jnp.exp(jax.random.uniform(second, (B, 1), jnp.float32) * jnp.log(10.0))
    ramp = jnp.arange(D, dtype=jnp.float32)[None, :] / D
    power = 0.24 * ramp + 0.76 * jax.random.uniform(third, (1, D), jnp.float32)
    col_scale = jnp.exp(power * jnp.log(10.0))
    return (base * row_scale * col_scale).astype(jnp.bfloat16)


def draw_lengths(key, part):
    first, second = jax.random.split(jax.random.fold_in(key, 4))
    values = jax.random.randint(first, (B,), 1, CTX + 1, jnp.int32)
    chosen = jax.random.randint(second, (), 0, B, jnp.int32)
    return jnp.where(jnp.arange(B, dtype=jnp.int32) == chosen, CTX, values).astype(jnp.int32)


def block_scale(stream_key, extent, cuts, least, top_value):
    level = 1.0
    for dim, blocks in cuts:
        steps = jax.random.uniform(jax.random.fold_in(jax.random.fold_in(stream_key, 6), dim), (blocks,), jnp.float32, least / len(cuts), top_value / len(cuts))
        level = level * jnp.repeat(jnp.exp(steps), extent[dim] // blocks).reshape((-1,) + (1,) * (len(extent) - 1 - dim))
    return level


def bell_draw(key, shape, scale, limit, shards=(), kind=jnp.bfloat16):
    gain = block_scale(key, shape, shards, -0.22, 0.18) if shards else 1.0
    entries = jax.random.normal(key, shape, jnp.float32) * scale * gain
    return jnp.minimum(jnp.maximum(entries, -limit), limit).astype(kind)


def setup_inputs(seed: int = 0, part: int = 0) -> dict:
    key_list = jax.random.split(jax.random.key(seed), 10)
    part_keys = jax.random.split(jax.random.fold_in(key_list[9], part), 10)
    hidden_in = draw_hidden_in(jax.random.fold_in(jax.random.fold_in(key_list[9], part), 71), part)
    norm_gain_vector = jnp.clip(1.0 + 0.18 * jax.random.normal(key_list[1], (D,), jnp.float32), 0.099609375, 1.8984375).astype(jnp.bfloat16)
    w_query = bell_draw(key_list[2], (D, QW), D ** -0.5, 0.09375, ((0, 4), (1, 2)))
    key_cache_rows = draw_key_cache_rows(jax.random.fold_in(jax.random.fold_in(key_list[9], part), 71), part)
    value_cache_rows = bell_draw(part_keys[4], (B, CTX, HD), 1.0, 6.0, ((0, 2), (1, 4)))
    k_new = draw_k_new(jax.random.fold_in(jax.random.fold_in(key_list[9], part), 71), part)
    v_new = bell_draw(part_keys[6], (B, HD), 1.0, 6.0, ((0, 2),))
    lengths = draw_lengths(jax.random.fold_in(jax.random.fold_in(key_list[9], part), 71), part)
    w_out = bell_draw(key_list[8], (QW, D), QW ** -0.5, 0.09375, ((0, 2), (1, 4)))
    return dict(hidden_in=hidden_in, norm_gain_vector=norm_gain_vector, w_query=w_query, key_cache_rows=key_cache_rows, value_cache_rows=value_cache_rows, k_new=k_new, v_new=v_new, lengths=lengths, w_out=w_out)


def reference(hidden_in, norm_gain_vector, w_query, key_cache_rows, value_cache_rows, k_new, v_new, lengths, w_out):
    inputs = hidden_in.astype(jnp.float32)
    mean_sq = lax.optimization_barrier(jnp.mean(inputs * inputs, axis=-1, keepdims=True))
    normed = (inputs * lax.rsqrt(mean_sq + 1e-05) * norm_gain_vector.astype(jnp.float32)).astype(jnp.bfloat16)
    inverse_root_norm = 1.0 / HD ** 0.5
    query_vectors = (jnp.dot(normed, w_query, preferred_element_type=jnp.float32) * inverse_root_norm).astype(jnp.bfloat16)
    query_vectors = query_vectors.reshape(query_vectors.shape[0], HQ, HD)

    def attend(per_seq):
        query_rows, key_rows, value_rows, used, key_own, value_own = per_seq
        scores = jnp.dot(query_rows, key_rows.T, preferred_element_type=jnp.float32)
        own = jnp.dot(query_rows, key_own, preferred_element_type=jnp.float32)
        live_mask = lax.iota(jnp.int32, key_rows.shape[0]) < used
        top = jnp.maximum(lax.optimization_barrier(jnp.max(jnp.where(live_mask[None, :], scores, -jnp.inf), axis=-1)), own)
        softmax_weights = jnp.where(live_mask[None, :], jnp.exp(scores - top[:, None]), jnp.float32(0.0))
        fresh = jnp.exp(own - top)
        totals = lax.optimization_barrier(jnp.sum(softmax_weights, axis=-1)) + fresh
        summed = jnp.dot(softmax_weights.astype(jnp.bfloat16), value_rows, preferred_element_type=jnp.float32)
        result = (summed + fresh[:, None] * value_own.astype(jnp.float32)[None, :]) / totals[:, None]
        return result.astype(jnp.bfloat16).reshape(HQ * HD)
    attended = lax.map(attend, (query_vectors, key_cache_rows, value_cache_rows, lengths, k_new, v_new))
    return jnp.dot(attended, w_out, preferred_element_type=jnp.float32)
```

```python
import functools

import jax
import jax.numpy as jnp
from jax import lax
from jax.experimental import pallas as pl
from jax.experimental.pallas import tpu as pltpu
from jax.sharding import PartitionSpec as P

HD = 128
EPS = 1e-05
MESH = pl.DeviceIdType.MESH
F32 = jnp.float32
BF16 = jnp.bfloat16


def chunk_edges(heads, cuts):
    step = heads // cuts
    return [(c * step, (c + 1) * step) for c in range(cuts)]


def kernel(
    n,
    heads,
    rows,
    cuts,
    lens_ref,
    hidden_hbm,
    gain_hbm,
    wq_hbm,
    keys_hbm,
    values_hbm,
    knew_hbm,
    vnew_hbm,
    wout_hbm,
    out_ref,
    hid,
    gain,
    wq,
    kbuf,
    vbuf,
    knew,
    vnew,
    wout,
    newf,
    qsend,
    qrecv,
    qall,
    asend,
    arecv,
    att,
    hsend,
    hrecv,
    small_sem,
    wq_sem,
    k_sem,
    v_sem,
    wo_sem,
    qs_send,
    qs_recv,
    qg_send,
    qg_recv,
    as_send,
    as_recv,
    ag_send,
    ag_recv,
    h_send,
    h_recv,
):
    me = lax.axis_index("seq")
    core = lax.axis_index("head")
    share = rows // n
    block = keys_hbm.shape[1]
    width = wq_hbm.shape[0] * n
    edges = chunk_edges(heads, cuts)

    small = [
        pltpu.make_async_copy(src, dst, small_sem.at[i])
        for i, (src, dst) in enumerate(
            ((hidden_hbm, hid), (gain_hbm, gain), (knew_hbm, knew), (vnew_hbm, vnew))
        )
    ]
    for copy in small:
        copy.start()
    wq_copies = []
    for c, (lo, hi) in enumerate(edges):
        cols = pl.ds(lo * HD, (hi - lo) * HD)
        wq_copies.append(pltpu.make_async_copy(wq_hbm.at[:, cols], wq.at[:, cols], wq_sem.at[c]))
        wq_copies[-1].start()
    owners = [lax.rem(me - k + n, n) for k in range(n)]
    k_copies, v_copies = [], []
    for k in range(n):
        group = pl.ds(owners[k] * share, share)
        k_copies.append(pltpu.make_async_copy(keys_hbm.at[group], kbuf.at[k], k_sem.at[k]))
        v_copies.append(pltpu.make_async_copy(values_hbm.at[group], vbuf.at[k], v_sem.at[k]))
        k_copies[-1].start()
        v_copies[-1].start()
    half = wout_hbm.shape[1] // 2
    wo_copies = []
    for i, side in enumerate((1 - core, core)):
        cols = pl.ds(pl.multiple_of(side * half, HD), half)
        wo_copies.append(pltpu.make_async_copy(wout_hbm.at[:, cols], wout.at[i], wo_sem.at[i]))
        wo_copies[-1].start()

    barrier = pltpu.get_barrier_semaphore()
    for k in range(1, n):
        pl.semaphore_signal(
            barrier, inc=1, device_id={"seq": lax.rem(me + k, n)}, device_id_type=MESH
        )
    pl.semaphore_signal(barrier, inc=1, device_id={"head": 1 - core}, device_id_type=MESH)

    small[0].wait()
    small[1].wait()
    x = hid[...].astype(F32)
    squares = jnp.sum(x * x, axis=-1, keepdims=True)
    scaled = x * gain[...].astype(F32)
    upper = scaled.astype(BF16)
    lower = (scaled - upper.astype(F32)).astype(BF16)
    both = jnp.concatenate([upper, lower], axis=0)
    for p in range(n):
        qsend[p, 0] = jnp.broadcast_to(squares[p * share : (p + 1) * share], (share, HD))
    qs = [[None] * n for _ in edges]
    for c, (lo, hi) in enumerate(edges):
        wq_copies[c].wait()
        product = jnp.dot(both, wq[:, lo * HD : hi * HD], preferred_element_type=F32)
        part = product[:rows] + product[rows:]
        for h in range(lo, hi):
            for p in range(n):
                qsend[p, h + 1] = part[
                    p * share : (p + 1) * share, (h - lo) * HD : (h - lo + 1) * HD
                ]
        if c == 0:
            pl.semaphore_wait(barrier, n)
        first = 0 if c == 0 else lo + 1
        span = pl.ds(first, hi + 1 - first)
        for k in range(1, n):
            peer = lax.rem(me + k, n)
            qs[c][k] = pltpu.make_async_remote_copy(
                src_ref=qsend.at[peer, span],
                dst_ref=qrecv.at[k - 1, span],
                send_sem=qs_send.at[c, k - 1],
                recv_sem=qs_recv.at[c, k - 1],
                device_id={"seq": peer},
                device_id_type=MESH,
            )
            qs[c][k].start()

    small[2].wait()
    small[3].wait()
    newf[0] = knew[...].astype(F32)
    newf[1] = vnew[...].astype(F32)

    for c in range(len(edges)):
        for k in range(1, n):
            qs[c][k].wait_recv()
    total = qsend[me]
    for k in range(1, n):
        total = total + qrecv[k - 1]
    inv = lax.rsqrt(total[0] / width + EPS) * (1.0 / HD**0.5)
    query = (total[1:] * inv[None]).astype(BF16).astype(F32)
    for r in range(share):
        qall[0, r] = jnp.concatenate([query[h, r : r + 1] for h in range(heads)], axis=0)
    qg = [None] * n
    for k in range(1, n):
        qg[k] = pltpu.make_async_remote_copy(
            src_ref=qall.at[0],
            dst_ref=qall.at[k],
            send_sem=qg_send.at[k - 1],
            recv_sem=qg_recv.at[k - 1],
            device_id={"seq": lax.rem(me + k, n)},
            device_id_type=MESH,
        )
        qg[k].start()

    lanes = lax.broadcasted_iota(jnp.int32, (heads, HD), 1)
    positions = me * block + lax.broadcasted_iota(jnp.int32, (heads, block), 1)
    sends = [None] * n
    for k in range(n):
        if k:
            qg[k].wait_recv()
        k_copies[k].wait()
        scores, own = [], []
        for r in range(share):
            q = qall[k, r]
            scores.append(
                lax.dot_general(
                    q.astype(BF16),
                    kbuf[k, r],
                    (((1,), (1,)), ((), ())),
                    preferred_element_type=F32,
                )
            )
            own.append(
                jnp.sum(q * newf[0, pl.ds(owners[k] * share + r, 1)], axis=-1, keepdims=True)
            )
        v_copies[k].wait()
        stats = jnp.zeros((heads, HD), F32)
        for r in range(share):
            live = positions < lens_ref[owners[k] * share + r]
            masked = jnp.where(live, scores[r], -jnp.inf)
            top = jnp.maximum(jnp.max(masked, axis=-1, keepdims=True), own[r])
            weights = jnp.exp(masked - top)
            stats = jnp.where(lanes == 2 * r, top, stats)
            stats = jnp.where(lanes == 2 * r + 1, jnp.sum(weights, axis=-1, keepdims=True), stats)
            asend[k, r] = jnp.dot(weights.astype(BF16), vbuf[k, r], preferred_element_type=F32)
        asend[k, share] = stats
        if k:
            sends[k] = pltpu.make_async_remote_copy(
                src_ref=asend.at[k],
                dst_ref=arecv.at[k - 1],
                send_sem=as_send.at[k - 1],
                recv_sem=as_recv.at[k - 1],
                device_id={"seq": owners[k]},
                device_id_type=MESH,
            )
            sends[k].start()

    for k in range(1, n):
        sends[k].wait_recv()
    stats = [asend[0, share]] + [arecv[k - 1, share] for k in range(1, n)]
    for r in range(share):
        tops = [s[:, 2 * r : 2 * r + 1] for s in stats]
        own = jnp.sum(qall[0, r] * newf[0, pl.ds(me * share + r, 1)], axis=-1, keepdims=True)
        top = functools.reduce(jnp.maximum, tops)
        fresh = jnp.exp(own - top)
        totals = fresh
        summed = fresh * newf[1, pl.ds(me * share + r, 1)]
        for k in range(n):
            factor = jnp.exp(tops[k] - top)
            totals = totals + stats[k][:, 2 * r + 1 : 2 * r + 2] * factor
            summed = summed + (asend[0, r] if k == 0 else arecv[k - 1, r]) * factor
        att[me * share + r] = (summed / totals).astype(BF16).astype(F32)
    ag = [None] * n
    mine = att.at[pl.ds(me * share, share)]
    for k in range(1, n):
        ag[k] = pltpu.make_async_remote_copy(
            src_ref=mine,
            dst_ref=mine,
            send_sem=ag_send.at[k - 1],
            recv_sem=ag_recv.at[k - 1],
            device_id={"seq": lax.rem(me + k, n)},
            device_id_type=MESH,
        )
        ag[k].start()
    for copy in wo_copies:
        copy.wait()
    for k in range(1, n):
        ag[k].wait_recv()

    attended = jnp.concatenate([att[:, h, :] for h in range(heads)], axis=1).astype(BF16)
    hsend[...] = jnp.dot(attended, wout[0], preferred_element_type=F32)
    swap = pltpu.make_async_remote_copy(
        src_ref=hsend,
        dst_ref=hrecv,
        send_sem=h_send,
        recv_sem=h_recv,
        device_id={"head": 1 - core},
        device_id_type=MESH,
    )
    swap.start()
    kept = jnp.dot(attended, wout[1], preferred_element_type=F32)
    swap.wait_recv()
    out_ref[...] = kept + hrecv[...]

    for k in range(1, n):
        for c in range(len(edges)):
            qs[c][k].wait_send()
        qg[k].wait_send()
        sends[k].wait_send()
        ag[k].wait_send()
    swap.wait_send()


def solution(mesh):
    n = mesh.shape["seq"]
    cuts = 2

    def shards(hidden, gain, wq, keys, values, knew, vnew, lengths, wout):
        rows, depth = hidden.shape
        heads = wq.shape[1] // HD
        share = rows // n
        block = keys.shape[1]
        half = wout.shape[1] // 2
        anywhere = pl.BlockSpec(memory_space=pl.ANY)
        dma = pltpu.SemaphoreType.DMA
        return pl.pallas_call(
            functools.partial(kernel, n, heads, rows, cuts),
            out_shape=jax.ShapeDtypeStruct((rows, half), F32),
            in_specs=[pl.BlockSpec(memory_space=pltpu.SMEM)] + [anywhere] * 8,
            out_specs=pl.BlockSpec(memory_space=pltpu.VMEM),
            scratch_shapes=[
                pltpu.VMEM((rows, depth), BF16),
                pltpu.VMEM((1, depth), BF16),
                pltpu.VMEM(wq.shape, BF16),
                pltpu.VMEM((n, share, block, HD), BF16),
                pltpu.VMEM((n, share, block, HD), BF16),
                pltpu.VMEM((rows, HD), BF16),
                pltpu.VMEM((rows, HD), BF16),
                pltpu.VMEM((2, wout.shape[0], half), BF16),
                pltpu.VMEM((2, rows, HD), F32),
                pltpu.VMEM((n, heads + 1, share, HD), F32),
                pltpu.VMEM((n - 1, heads + 1, share, HD), F32),
                pltpu.VMEM((n, share, heads, HD), F32),
                pltpu.VMEM((n, share + 1, heads, HD), F32),
                pltpu.VMEM((n - 1, share + 1, heads, HD), F32),
                pltpu.VMEM((rows, heads, HD), F32),
                pltpu.VMEM((rows, half), F32),
                pltpu.VMEM((rows, half), F32),
                dma((4,)),
                dma((cuts,)),
                dma((n,)),
                dma((n,)),
                dma((2,)),
                dma((cuts, n - 1)),
                dma((cuts, n - 1)),
                dma((n - 1,)),
                dma((n - 1,)),
                dma((n - 1,)),
                dma((n - 1,)),
                dma((n - 1,)),
                dma((n - 1,)),
                dma(()),
                dma(()),
            ],
            compiler_params=pltpu.CompilerParams(collective_id=0, has_side_effects=True),
            name="decode_step",
        )(lengths, hidden, gain.reshape(1, -1), wq, keys, values, knew, vnew, wout)

    placed = (
        P(("groups", "batch"), "seq"),
        P("seq"),
        P("seq", "head"),
        P(("groups", "batch"), "seq", None),
        P(("groups", "batch"), "seq", None),
        P(("groups", "batch"), None),
        P(("groups", "batch"), None),
        P(("groups", "batch")),
        P("head", "seq"),
    )
    return jax.shard_map(
        shards,
        mesh=mesh,
        in_specs=placed,
        out_specs=P(("groups", "batch"), ("seq", "head")),
        check_vma=False,
    )
```

```python
import functools

import jax
import jax.numpy as jnp
from jax import lax
from jax.experimental import pallas as pl
from jax.experimental.pallas import tpu as pltpu
from jax.sharding import PartitionSpec as P

HD = 128
EPS = 1e-05
MESH = pl.DeviceIdType.MESH
F32 = jnp.float32
BF16 = jnp.bfloat16


def chunk_edges(heads, cuts):
    step = heads // cuts
    return [(c * step, (c + 1) * step) for c in range(cuts)]


def kernel(
    n,
    heads,
    rows,
    cuts,
    m,
    subs,
    lens_ref,
    hidden_hbm,
    gain_hbm,
    wq_hbm,
    keys_hbm,
    values_hbm,
    knew_hbm,
    vnew_hbm,
    wout_hbm,
    out_ref,
    hid,
    gain,
    wq,
    kbuf,
    vbuf,
    knew,
    vnew,
    wout,
    newf,
    qsend,
    qrecv,
    qturn,
    qall,
    asend,
    arecv,
    att,
    hsend,
    hrecv,
    small_sem,
    wq_sem,
    k_sem,
    v_sem,
    wo_sem,
    qs_send,
    qs_recv,
    qg_send,
    qg_recv,
    as_send,
    as_recv,
    ag_send,
    ag_recv,
    h_send,
    h_recv,
):
    me = lax.axis_index("seq")
    core = lax.axis_index("head")
    other = 1 - core
    first = (n - m) // 2
    share = rows // m
    piece = share // subs
    block = keys_hbm.shape[1]
    width = wq_hbm.shape[0] * n
    edges = chunk_edges(heads, cuts)
    owning = jnp.logical_and(me >= first, me < first + m)
    my_slot = jnp.clip(me - first, 0, m - 1)
    slots = [lax.rem(my_slot + k, m) for k in range(m)]
    away = [(n // 2 + k) % n for k in range(n)]
    away = [k for k in away if k]

    barrier = pltpu.get_barrier_semaphore()

    def greet(s):
        pl.semaphore_signal(
            barrier, inc=1, device_id={"seq": s, "head": core}, device_id_type=MESH
        )

    for s in range(n):
        meet = me != s
        if not first <= s < first + m:
            meet = jnp.logical_and(meet, owning)
        pl.when(meet)(functools.partial(greet, s))
    pl.semaphore_signal(barrier, inc=1, device_id={"head": other}, device_id_type=MESH)

    small = [
        pltpu.make_async_copy(src, dst, small_sem.at[i])
        for i, (src, dst) in enumerate(
            ((hidden_hbm, hid), (gain_hbm, gain), (knew_hbm, knew), (vnew_hbm, vnew))
        )
    ]
    for copy in small:
        copy.start()
    wq_copies = []
    for c, (lo, hi) in enumerate(edges):
        cols = pl.ds(lo * HD, (hi - lo) * HD)
        wq_copies.append(pltpu.make_async_copy(wq_hbm.at[:, cols], wq.at[:, cols], wq_sem.at[c]))
        wq_copies[-1].start()
    k_copies, v_copies = [], []
    for k in range(m):
        group = pl.ds(slots[k] * share, share)
        k_copies.append(pltpu.make_async_copy(keys_hbm.at[group], kbuf.at[k], k_sem.at[k]))
        v_copies.append(pltpu.make_async_copy(values_hbm.at[group], vbuf.at[k], v_sem.at[k]))
        k_copies[-1].start()
        v_copies[-1].start()
    half = wout_hbm.shape[1] // 2
    wo_copies = []
    for i, side in enumerate((other, core)):
        cols = pl.ds(pl.multiple_of(side * half, HD), half)
        wo_copies.append(pltpu.make_async_copy(wout_hbm.at[:, cols], wout.at[i], wo_sem.at[i]))
        wo_copies[-1].start()

    small[0].wait()
    small[1].wait()
    x = hid[...].astype(F32)
    squares = jnp.sum(x * x, axis=-1, keepdims=True)
    scaled = x * gain[...].astype(F32)
    upper = scaled.astype(BF16)
    lower = (scaled - upper.astype(F32)).astype(BF16)
    both = jnp.concatenate([upper, lower], axis=0)
    for p in range(m):
        qsend[p, 0] = jnp.broadcast_to(squares[p * share : (p + 1) * share], (share, HD))
    qs = [[None] * m for _ in edges]

    def arrivals(c, s):
        lo, hi = edges[c]
        span = pl.ds(0 if c == 0 else lo + 1, hi + 1 - (0 if c == 0 else lo + 1))
        return pltpu.make_async_remote_copy(
            src_ref=qsend.at[0, span],
            dst_ref=qrecv.at[s, span],
            send_sem=qs_send.at[c, 0],
            recv_sem=qs_recv.at[c, s],
            device_id={"seq": me, "head": core},
            device_id_type=MESH,
        )

    for c, (lo, hi) in enumerate(edges):
        wq_copies[c].wait()
        product = jnp.dot(both, wq[:, lo * HD : hi * HD], preferred_element_type=F32)
        part = product[:rows] + product[rows:]
        for h in range(lo, hi):
            for p in range(m):
                qsend[p, h + 1] = part[
                    p * share : (p + 1) * share, (h - lo) * HD : (h - lo + 1) * HD
                ]
        if c == 0:
            pl.semaphore_wait(barrier, jnp.where(owning, n, m + 1))
        start = 0 if c == 0 else lo + 1
        span = pl.ds(start, hi + 1 - start)
        for k in reversed(range(m)):
            qs[c][k] = pltpu.make_async_remote_copy(
                src_ref=qsend.at[slots[k], span],
                dst_ref=qrecv.at[me, span],
                send_sem=qs_send.at[c, k],
                recv_sem=qs_recv.at[c, me],
                device_id={"seq": slots[k] + first, "head": core},
                device_id_type=MESH,
            )
            if k:
                qs[c][k].start()
            else:
                pl.when(jnp.logical_not(owning))(qs[c][k].start)

    small[2].wait()
    small[3].wait()
    newf[0] = knew[...].astype(F32)
    newf[1] = vnew[...].astype(F32)

    def gathers(u):
        return [
            pltpu.make_async_remote_copy(
                src_ref=qall.at[my_slot, pl.ds(u * piece, piece)],
                dst_ref=qall.at[my_slot, pl.ds(u * piece, piece)],
                send_sem=qg_send.at[u, i],
                recv_sem=qg_recv.at[u, my_slot],
                device_id={"seq": lax.rem(me + k, n), "head": core},
                device_id_type=MESH,
            )
            for i, k in enumerate(away)
        ]

    @pl.when(owning)
    def _():
        for c in range(len(edges)):
            for s in range(1, n):
                arrivals(c, lax.rem(me + s, n)).wait_recv()
        total = qsend[my_slot]
        for s in range(1, n):
            total = total + qrecv[lax.rem(me + s, n)]
        inv = lax.rsqrt(total[0] / width + EPS) * (1.0 / HD**0.5)
        qturn[...] = (total[1:] * inv[None]).astype(BF16).astype(F32)
        for u in range(subs):
            for r in range(u * piece, (u + 1) * piece):
                qall[my_slot, r] = qturn[:, r, :]
            for copy in gathers(u):
                copy.start()

    lanes = lax.broadcasted_iota(jnp.int32, (heads, HD), 1)
    positions = me * block + lax.broadcasted_iota(jnp.int32, (heads, block), 1)
    sends = []
    for k in range(m):
        for u in range(subs):
            i = k * subs + u
            arrival = pltpu.make_async_remote_copy(
                src_ref=qall.at[my_slot, pl.ds(u * piece, piece)],
                dst_ref=qall.at[slots[k], pl.ds(u * piece, piece)],
                send_sem=qg_send.at[u, 0],
                recv_sem=qg_recv.at[u, slots[k]],
                device_id={"seq": me, "head": core},
                device_id_type=MESH,
            )
            if k:
                arrival.wait_recv()
            else:
                pl.when(jnp.logical_not(owning))(arrival.wait_recv)
            if u == 0:
                k_copies[k].wait()
            scores, own = [], []
            for r in range(piece):
                q = qall[slots[k], u * piece + r]
                scores.append(
                    lax.dot_general(
                        q.astype(BF16),
                        kbuf[k, u * piece + r],
                        (((1,), (1,)), ((), ())),
                        preferred_element_type=F32,
                    )
                )
                row = slots[k] * share + u * piece + r
                own.append(jnp.sum(q * newf[0, pl.ds(row, 1)], axis=-1, keepdims=True))
            if u == 0:
                v_copies[k].wait()
            stats = jnp.zeros((heads, HD), F32)
            for r in range(piece):
                live = positions < lens_ref[slots[k] * share + u * piece + r]
                masked = jnp.where(live, scores[r], -jnp.inf)
                top = jnp.maximum(jnp.max(masked, axis=-1, keepdims=True), own[r])
                weights = jnp.exp(masked - top)
                weight = jnp.sum(weights, axis=-1, keepdims=True)
                stats = jnp.where(lanes == 2 * r, top, stats)
                stats = jnp.where(lanes == 2 * r + 1, weight, stats)
                asend[i, r] = jnp.dot(
                    weights.astype(BF16), vbuf[k, u * piece + r], preferred_element_type=F32
                )
            asend[i, piece] = stats
            sends.append(
                pltpu.make_async_remote_copy(
                    src_ref=asend.at[i],
                    dst_ref=arecv.at[me, u],
                    send_sem=as_send.at[i],
                    recv_sem=as_recv.at[u, me],
                    device_id={"seq": slots[k] + first, "head": core},
                    device_id_type=MESH,
                )
            )
            if k:
                sends[-1].start()
            else:
                pl.when(jnp.logical_not(owning))(sends[-1].start)

    def returns(u):
        return [
            pltpu.make_async_remote_copy(
                src_ref=att.at[pl.ds(my_slot * share + u * piece, piece)],
                dst_ref=att.at[pl.ds(my_slot * share + u * piece, piece)],
                send_sem=ag_send.at[u, i],
                recv_sem=ag_recv.at[u, my_slot],
                device_id={"seq": lax.rem(me + k, n), "head": core},
                device_id_type=MESH,
            )
            for i, k in enumerate(away)
        ]

    @pl.when(owning)
    def _():
        for u in range(subs):
            others = [lax.rem(me + s, n) for s in range(1, n)]
            for s in others:
                pltpu.make_async_remote_copy(
                    src_ref=asend.at[0],
                    dst_ref=arecv.at[s, u],
                    send_sem=as_send.at[0],
                    recv_sem=as_recv.at[u, s],
                    device_id={"seq": me, "head": core},
                    device_id_type=MESH,
                ).wait_recv()
            stats = [asend[u, piece]] + [arecv[s, u, piece] for s in others]
            for r in range(piece):
                row = my_slot * share + u * piece + r
                tops = [s[:, 2 * r : 2 * r + 1] for s in stats]
                own = jnp.sum(
                    qall[my_slot, u * piece + r] * newf[0, pl.ds(row, 1)], axis=-1, keepdims=True
                )
                top = functools.reduce(jnp.maximum, tops)
                fresh = jnp.exp(own - top)
                totals = fresh
                summed = fresh * newf[1, pl.ds(row, 1)]
                for s in range(n):
                    factor = jnp.exp(tops[s] - top)
                    totals = totals + stats[s][:, 2 * r + 1 : 2 * r + 2] * factor
                    summed = summed + (arecv[others[s - 1], u, r] if s else asend[u, r]) * factor
                att[row] = (summed / totals).astype(BF16).astype(F32)
            for copy in returns(u):
                copy.start()

    for copy in wo_copies:
        copy.wait()
    for j in range(m):
        for u in range(subs):
            group = pl.ds(j * share + u * piece, piece)
            arrival = pltpu.make_async_remote_copy(
                src_ref=att.at[group],
                dst_ref=att.at[group],
                send_sem=ag_send.at[u, 0],
                recv_sem=ag_recv.at[u, j],
                device_id={"seq": me, "head": core},
                device_id_type=MESH,
            )
            pl.when(me != first + j)(arrival.wait_recv)

    attended = jnp.concatenate([att[:, h, :] for h in range(heads)], axis=1).astype(BF16)
    hsend[...] = jnp.dot(attended, wout[0], preferred_element_type=F32)
    swap = pltpu.make_async_remote_copy(
        src_ref=hsend,
        dst_ref=hrecv,
        send_sem=h_send,
        recv_sem=h_recv,
        device_id={"head": other},
        device_id_type=MESH,
    )
    swap.start()
    kept = jnp.dot(attended, wout[1], preferred_element_type=F32)
    swap.wait_recv()
    out_ref[...] = kept + hrecv[...]

    for c in range(len(edges)):
        for k in range(1, m):
            qs[c][k].wait_send()
    for copy in sends[subs:]:
        copy.wait_send()
    swap.wait_send()

    @pl.when(owning)
    def _():
        for u in range(subs):
            for copy in gathers(u) + returns(u):
                copy.wait_send()

    @pl.when(jnp.logical_not(owning))
    def _():
        for c in range(len(edges)):
            qs[c][0].wait_send()
        for copy in sends[:subs]:
            copy.wait_send()


def solution(mesh):
    n = mesh.shape["seq"]
    cuts = 2
    m = max(n // 2, 1)
    subs = 2

    def shards(hidden, gain, wq, keys, values, knew, vnew, lengths, wout):
        rows, depth = hidden.shape
        heads = wq.shape[1] // HD
        share = rows // m
        piece = share // subs
        block = keys.shape[1]
        half = wout.shape[1] // 2
        anywhere = pl.BlockSpec(memory_space=pl.ANY)
        dma = pltpu.SemaphoreType.DMA
        return pl.pallas_call(
            functools.partial(kernel, n, heads, rows, cuts, m, subs),
            out_shape=jax.ShapeDtypeStruct((rows, half), F32),
            in_specs=[pl.BlockSpec(memory_space=pltpu.SMEM)] + [anywhere] * 8,
            out_specs=pl.BlockSpec(memory_space=pltpu.VMEM),
            scratch_shapes=[
                pltpu.VMEM((rows, depth), BF16),
                pltpu.VMEM((1, depth), BF16),
                pltpu.VMEM(wq.shape, BF16),
                pltpu.VMEM((m, share, block, HD), BF16),
                pltpu.VMEM((m, share, block, HD), BF16),
                pltpu.VMEM((rows, HD), BF16),
                pltpu.VMEM((rows, HD), BF16),
                pltpu.VMEM((2, wout.shape[0], half), BF16),
                pltpu.VMEM((2, rows, HD), F32),
                pltpu.VMEM((m, heads + 1, share, HD), F32),
                pltpu.VMEM((n, heads + 1, share, HD), F32),
                pltpu.VMEM((heads, share, HD), F32),
                pltpu.VMEM((m, share, heads, HD), F32),
                pltpu.VMEM((m * subs, piece + 1, heads, HD), F32),
                pltpu.VMEM((n, subs, piece + 1, heads, HD), F32),
                pltpu.VMEM((rows, heads, HD), F32),
                pltpu.VMEM((rows, half), F32),
                pltpu.VMEM((rows, half), F32),
                dma((4,)),
                dma((cuts,)),
                dma((m,)),
                dma((m,)),
                dma((2,)),
                dma((cuts, m)),
                dma((cuts, n)),
                dma((subs, n)),
                dma((subs, m)),
                dma((m * subs,)),
                dma((subs, n)),
                dma((subs, n)),
                dma((subs, m)),
                dma(()),
                dma(()),
            ],
            compiler_params=pltpu.CompilerParams(collective_id=0, has_side_effects=True),
            name="decode_step",
        )(lengths, hidden, gain.reshape(1, -1), wq, keys, values, knew, vnew, wout)

    placed = (
        P(("groups", "batch"), "seq"),
        P("seq"),
        P("seq", "head"),
        P(("groups", "batch"), "seq", None),
        P(("groups", "batch"), "seq", None),
        P(("groups", "batch"), None),
        P(("groups", "batch"), None),
        P(("groups", "batch")),
        P("head", "seq"),
    )
    return jax.shard_map(
        shards,
        mesh=mesh,
        in_specs=placed,
        out_specs=P(("groups", "batch"), ("seq", "head")),
        check_vma=False,
    )
```
